8 devices in a mesh: stage: 2 (over z, y), data: 4 (over x, core).
Axes of the slice: x: 2, y: 2, z: 1, core: 2. Of those that a mesh axis runs over, the one named last changes fastest.
Arguments:
- inputs: bfloat16 [16, 512, 1600], P('data')
- targets: bfloat16 [16, 512, 1600], P('data')
- w_up: bfloat16 [8, 1600, 6400], P('stage')
- w_down: bfloat16 [8, 6400, 1600], P('stage')
Outputs:
- output 1: float32 [], replicated
- output 2: float32 [8, 1600, 6400], P('stage', 'data')
- output 3: float32 [8, 6400, 1600], P('stage', None, 'data')
All inputs are finite; a program needn't handle non-finite values.
Results may differ from the reference program's by a relative error of at most 0.00342528.
Values are sent between devices in bfloat16 or wider.
A program may use at most 1 GiB of HBM per device.

```python
import jax
import jax.numpy as jnp
from jax import lax

DATA_REPLICAS = 4
MICRO = 4
TOKENS = 512
D_MODEL = 1600
FFN = 6400
LAYERS = 8


def setup_inputs(seed: int = 0) -> dict:
    root_key = jax.random.key(seed)
    key_inputs, key_targets, key_up, key_down = jax.random.split(root_key, 4)
    n_rows = DATA_REPLICAS * MICRO
    inputs = jax.random.normal(key_inputs, (n_rows, TOKENS, D_MODEL), jnp.float32)
    targets = jax.random.normal(key_targets, (n_rows, TOKENS, D_MODEL), jnp.float32)
    w_up = jax.random.normal(key_up, (LAYERS, D_MODEL, FFN), jnp.float32) * D_MODEL ** -0.5
    w_down = jax.random.normal(key_down, (LAYERS, FFN, D_MODEL), jnp.float32) * 1.5 * (FFN * LAYERS) ** -0.5
    return {'inputs': inputs.astype(jnp.bfloat16), 'targets': targets.astype(jnp.bfloat16), 'w_up': w_up.astype(jnp.bfloat16), 'w_down': w_down.astype(jnp.bfloat16)}


def layer_forward(h_in, w_up, w_down):
    pre_act = jnp.dot(h_in, w_up, preferred_element_type=jnp.float32)
    gelu_out = jax.nn.gelu(pre_act).astype(jnp.bfloat16)
    branch = jnp.dot(gelu_out, w_down, preferred_element_type=jnp.float32)
    return (h_in.astype(jnp.float32) + branch).astype(jnp.bfloat16)


def layer_backward(h_in, grad_out, w_up, w_down):
    pre_act = jnp.dot(h_in, w_up, preferred_element_type=jnp.float32)
    gelu_full, gelu_vjp = jax.vjp(jax.nn.gelu, pre_act)
    gelu_out = gelu_full.astype(jnp.bfloat16)
    g_down = jnp.dot(gelu_out.T, grad_out, preferred_element_type=jnp.float32)
    grad_act = jnp.dot(grad_out, w_down.T, preferred_element_type=jnp.float32).astype(jnp.bfloat16)
    grad_pre = gelu_vjp(grad_act.astype(jnp.float32))[0].astype(jnp.bfloat16)
    g_up = jnp.dot(h_in.T, grad_pre, preferred_element_type=jnp.float32)
    back_prod = jnp.dot(grad_pre, w_up.T, preferred_element_type=jnp.float32)
    grad_in = (grad_out.astype(jnp.float32) + back_prod).astype(jnp.bfloat16)
    return grad_in, g_up, g_down


def reference(inputs, targets, w_up, w_down):
    inv_total = 1.0 / (inputs.shape[0] * inputs.shape[1])

    def fwd_step(h_cur, weights):
        return layer_forward(h_cur, weights[0], weights[1]), h_cur

    def bwd_step(grad_cur, packed):
        grad_in, g_up, g_down = layer_backward(packed[0], grad_cur, packed[1], packed[2])
        return grad_in, (g_up, g_down)

    def one_micro(loop_state, mb_pair):
        acc_up, acc_down, loss_sum = loop_state
        h_last, layer_ins = lax.scan(fwd_step, mb_pair[0], (w_up, w_down))
        resid_diff = h_last.astype(jnp.float32) - mb_pair[1].astype(jnp.float32)
        top_grad = (resid_diff * inv_total).astype(jnp.bfloat16)
        scan_out = lax.scan(bwd_step, top_grad, (layer_ins, w_up, w_down), reverse=True)
        grads_up, grads_down = scan_out[1]
        new_state = (acc_up + grads_up, acc_down + grads_down, loss_sum + jnp.sum(resid_diff * resid_diff))
        return new_state, None

    init_state = (jnp.zeros(w_up.shape, jnp.float32), jnp.zeros(w_down.shape, jnp.float32), jnp.zeros((), jnp.float32))
    final_state = lax.scan(one_micro, init_state, (inputs, targets))[0]
    return final_state[2] * (0.5 * inv_total), final_state[0], final_state[1]
```

```python
import functools

import jax
import jax.numpy as jnp
from jax import lax
from jax.experimental import pallas as pl
from jax.experimental.pallas import tpu as pltpu
from jax.sharding import PartitionSpec as P

BF16 = jnp.bfloat16
F32 = jnp.float32
CHUNK = 256
TILE = 1280
SLOTS = 3
MESH = pl.DeviceIdType.MESH
NN = (((1,), (0,)), ((), ()))
NT = (((1,), (1,)), ((), ()))
GELU_A = 0.7978845608028654
GELU_B = 0.044715
VMEM_LIMIT = 66_000_000


def pipe_index(stage, data):
    return 4 * stage + lax.rem(data + 2 * stage, 4)


def pipe_device(pos):
    stage = lax.div(pos, 4)
    return {'stage': stage, 'data': lax.rem(pos + 2 * stage, 4)}


def remote(src, dst, send_sem, recv_sem, pos):
    return pltpu.make_async_remote_copy(
        src_ref=src, dst_ref=dst, send_sem=send_sem, recv_sem=recv_sem,
        device_id=pipe_device(pos), device_id_type=MESH)


def load_weights(layer, pairs, sems, n_tile):
    def copy(i, ref, buf, j):
        part = (slice(None), pl.ds(j * TILE, TILE))
        return pltpu.make_async_copy(ref.at[(layer,) + part], buf.at[part], sems.at[i, j])
    copies = [copy(i, ref, buf, j) for i, (ref, buf) in enumerate(pairs) for j in range(n_tile)]
    for c in copies:
        c.start()
    return copies


def cols(c):
    return pl.ds(pl.multiple_of(c * CHUNK, CHUNK), CHUNK)


def fwd_kernel(n_pos, n_chunk, inv_total,
               x_ref, y_ref, w1_ref, w2_ref,
               h_all, u_all, g_all, e_all, y_all, loss_ref,
               w1, w2, hbuf, hrow, ubuf, gbuf, acc, obuf, ybuf,
               w_sem, load_sem, store_sem, u_sem, g_sem, out_sem, y_load_sem,
               recv_sem, x_recv_sem, y_recv_sem, x_send_sem, y_send_sem, credit):
    stage = lax.axis_index('stage')
    data = lax.axis_index('data')
    pos = pipe_index(stage, data)
    last = n_pos - 1
    per = n_chunk // 4
    width, ffn = w1.shape
    n_tile = ffn // TILE

    weights = load_weights(lax.rem(pos, 4), ((w1_ref, w1), (w2_ref, w2)), w_sem, n_tile)

    def piece(ref, k):
        n_half = ref.shape[2] // CHUNK
        return ref.at[lax.div(k, n_half), :, cols(lax.rem(k, n_half))]

    def send_x(k):
        c = data * per + k
        return remote(piece(x_ref, k), h_all.at[:, cols(c)], x_send_sem.at[k], x_recv_sem.at[c], 0)

    def own_x(k):
        return pltpu.make_async_copy(piece(x_ref, k), h_all.at[:, cols(k)], x_recv_sem.at[k])

    def send_y(k):
        c = data * per + k
        return remote(piece(y_ref, k), y_all.at[:, cols(c)], y_send_sem.at[k], y_recv_sem.at[c], last)

    def own_y(k):
        c = data * per + k
        return pltpu.make_async_copy(piece(y_ref, k), y_all.at[:, cols(c)], y_recv_sem.at[c])

    def wait_x(c):
        k = lax.rem(c, per)
        remote(piece(x_ref, k), h_all.at[:, cols(c)], x_send_sem.at[k], x_recv_sem.at[c], 0).wait_recv()

    def wait_y(c):
        k = lax.rem(c, per)
        remote(piece(y_ref, k), y_all.at[:, cols(c)], y_send_sem.at[k], y_recv_sem.at[c], last).wait_recv()

    def load(c):
        slot = lax.rem(c, SLOTS)
        return pltpu.make_async_copy(h_all.at[:, cols(c)], hbuf.at[slot], load_sem.at[slot])

    def store(c):
        slot = lax.rem(c, SLOTS)
        return pltpu.make_async_copy(hbuf.at[slot], h_all.at[:, cols(c)], store_sem.at[slot])

    def send_h(c):
        slot = lax.rem(c, SLOTS)
        out = lax.rem(c, 2)
        return remote(obuf.at[out], hbuf.at[slot], out_sem.at[out], recv_sem.at[slot], pos + 1)

    def keep_e(c):
        out = lax.rem(c, 2)
        return pltpu.make_async_copy(obuf.at[out], e_all.at[:, cols(c)], out_sem.at[out])

    def u_store(c, j):
        part = pl.ds(j * TILE, TILE)
        return pltpu.make_async_copy(ubuf.at[:, part], u_all.at[cols(c), part], u_sem.at[j])

    def g_store(c, j):
        part = pl.ds(j * TILE, TILE)
        return pltpu.make_async_copy(gbuf.at[:, part], g_all.at[cols(c), part], g_sem.at[j])

    def y_load(c):
        return pltpu.make_async_copy(y_all.at[:, cols(c)], ybuf, y_load_sem)

    @pl.when(pos == 0)
    def _():
        @pl.loop(0, per)
        def _(k):
            own_x(k).start()

    @pl.when((stage == 0) & (pos != 0))
    def _():
        @pl.loop(0, per)
        def _(k):
            send_x(k).start()

    @pl.when(pos == last)
    def _():
        @pl.loop(0, per)
        def _(k):
            own_y(k).start()

    @pl.when((pos == 4) | (pos == 6))
    def _():
        @pl.loop(0, per)
        def _(k):
            send_y(k).start()

    for copy in weights:
        copy.wait()
    loss_ref[...] = jnp.zeros_like(loss_ref)

    @pl.when(pos == 0)
    def _():
        wait_x(0)
        load(0).start()

    @pl.loop(0, n_chunk)
    def _(c):
        slot = lax.rem(c, SLOTS)

        @pl.when(pos == 0)
        def _():
            load(c).wait()

            @pl.when(c + 1 < n_chunk)
            def _():
                wait_x(c + 1)
                load(c + 1).start()

        @pl.when(pos != 0)
        def _():
            send_h(c).wait_recv()
            store(c).start()

            @pl.when(c > 0)
            def _():
                store(c - 1).wait()

                @pl.when(c - 1 + SLOTS < n_chunk)
                def _():
                    pl.semaphore_signal(credit, inc=1, device_id=pipe_device(pos - 1), device_id_type=MESH)

        @pl.when(c > 0)
        def _():
            for j in range(n_tile):
                u_store(c - 1, j).wait()
                g_store(c - 1, j).wait()

        @pl.when(pos == last)
        def _():
            wait_y(c)
            y_load(c).start()

        hrow[...] = hbuf[slot].T
        acc[...] = hbuf[slot].astype(F32)
        for j in range(n_tile):
            part = slice(j * TILE, (j + 1) * TILE)
            u = lax.dot_general(hrow[...], w1[:, part], NN, preferred_element_type=F32)
            ubuf[:, part] = u
            t = jnp.tanh(GELU_A * (u + GELU_B * (u * u * u)))
            gbuf[:, part] = (0.5 * u * (1.0 + t)).astype(BF16)
            u_store(c, j).start()
            g_store(c, j).start()
            acc[...] += lax.dot_general(w2[:, part], gbuf[:, part], NT, preferred_element_type=F32)

        @pl.when(pos != last)
        def _():
            @pl.when(c > 1)
            def _():
                send_h(c - 2).wait_send()
            obuf[lax.rem(c, 2)] = acc[...].astype(BF16)

            @pl.when(c >= SLOTS)
            def _():
                pl.semaphore_wait(credit, 1)
            send_h(c).start()

        @pl.when(pos == last)
        def _():
            @pl.when(c > 1)
            def _():
                keep_e(c - 2).wait()
            y_load(c).wait()
            diff = acc[...].astype(BF16).astype(F32) - ybuf[...].astype(F32)
            loss_ref[...] += jnp.sum((diff * diff).reshape(width // 8, 8, CHUNK), axis=0)
            obuf[lax.rem(c, 2)] = (diff * inv_total).astype(BF16)
            keep_e(c).start()

        @pl.when((pos == 5) & (lax.rem(c, 3) == 1) & (c < 3 * per))
        def _():
            send_y(lax.div(c, 3)).start()

    for j in range(n_tile):
        u_store(n_chunk - 1, j).wait()
        g_store(n_chunk - 1, j).wait()

    @pl.when(pos != last)
    def _():
        for c in (n_chunk - 2, n_chunk - 1):
            send_h(c).wait_send()

    @pl.when(pos == last)
    def _():
        for c in (n_chunk - 2, n_chunk - 1):
            keep_e(c).wait()

    @pl.when(pos != 0)
    def _():
        store(n_chunk - 1).wait()

    @pl.when((stage == 0) & (pos != 0))
    def _():
        @pl.loop(0, per)
        def _(k):
            send_x(k).wait_send()

    @pl.when((stage == 1) & (pos != last))
    def _():
        @pl.loop(0, per)
        def _(k):
            send_y(k).wait_send()


def bwd_kernel(n_pos, n_chunk,
               w1_ref, w2_ref, u_all, e_in,
               q_all, e_all,
               w1, w2, ebuf, erow, ubuf, qbuf, acc, obuf,
               w_sem, load_sem, store_sem, u_sem, q_sem, out_sem, recv_sem, credit):
    stage = lax.axis_index('stage')
    data = lax.axis_index('data')
    pos = pipe_index(stage, data)
    last = n_pos - 1
    width, ffn = w1.shape
    n_tile = ffn // TILE

    def u_load(c, j):
        part = pl.ds(j * TILE, TILE)
        return pltpu.make_async_copy(u_all.at[cols(c), part], ubuf.at[:, part], u_sem.at[j])

    weights = load_weights(lax.rem(pos, 4), ((w2_ref, w2), (w1_ref, w1)), w_sem, n_tile)
    for j in range(n_tile):
        u_load(0, j).start()

    def load(c):
        slot = lax.rem(c, SLOTS)
        return pltpu.make_async_copy(e_all.at[:, cols(c)], ebuf.at[slot], load_sem.at[slot])

    def store(c):
        slot = lax.rem(c, SLOTS)
        return pltpu.make_async_copy(ebuf.at[slot], e_all.at[:, cols(c)], store_sem.at[slot])

    def send_e(c):
        slot = lax.rem(c, SLOTS)
        out = lax.rem(c, 2)
        return remote(obuf.at[out], ebuf.at[slot], out_sem.at[out], recv_sem.at[slot], pos - 1)

    def q_store(c, j):
        part = pl.ds(j * TILE, TILE)
        return pltpu.make_async_copy(qbuf.at[:, part], q_all.at[cols(c), part], q_sem.at[j])

    for copy in weights:
        copy.wait()

    @pl.when(pos == last)
    def _():
        load(0).start()

    @pl.loop(0, n_chunk)
    def _(c):
        slot = lax.rem(c, SLOTS)

        @pl.when(pos == last)
        def _():
            load(c).wait()

            @pl.when(c + 1 < n_chunk)
            def _():
                load(c + 1).start()

        @pl.when(pos != last)
        def _():
            send_e(c).wait_recv()
            store(c).start()

            @pl.when(c > 0)
            def _():
                store(c - 1).wait()

                @pl.when(c - 1 + SLOTS < n_chunk)
                def _():
                    pl.semaphore_signal(credit, inc=1, device_id=pipe_device(pos + 1), device_id_type=MESH)

        @pl.when(c > 0)
        def _():
            for j in range(n_tile):
                q_store(c - 1, j).wait()

        for j in range(n_tile):
            u_load(c, j).wait()

        erow[...] = ebuf[slot].T
        acc[...] = ebuf[slot].astype(F32)
        for j in range(n_tile):
            part = slice(j * TILE, (j + 1) * TILE)
            p = lax.dot_general(erow[...], w2[:, part], NN, preferred_element_type=F32)
            p = p.astype(BF16).astype(F32)
            u = ubuf[:, part]
            u2 = u * u
            t = jnp.tanh(GELU_A * (u + GELU_B * (u * u2)))
            slope = 0.5 * (1.0 + t) + (0.5 * u) * (1.0 - t * t) * (GELU_A * (1.0 + (3.0 * GELU_B) * u2))
            qbuf[:, part] = (p * slope).astype(BF16)
            q_store(c, j).start()

            @pl.when(c + 1 < n_chunk)
            def _():
                u_load(c + 1, j).start()
            acc[...] += lax.dot_general(w1[:, part], qbuf[:, part], NT, preferred_element_type=F32)

        @pl.when(pos != 0)
        def _():
            @pl.when(c > 1)
            def _():
                send_e(c - 2).wait_send()
            obuf[lax.rem(c, 2)] = acc[...].astype(BF16)

            @pl.when(c >= SLOTS)
            def _():
                pl.semaphore_wait(credit, 1)
            send_e(c).start()

    for j in range(n_tile):
        q_store(n_chunk - 1, j).wait()

    @pl.when(pos != last)
    def _():
        store(n_chunk - 1).wait()

    @pl.when(pos != 0)
    def _():
        for c in (n_chunk - 2, n_chunk - 1):
            send_e(c).wait_send()


def any_specs(n):
    return [pl.BlockSpec(memory_space=pl.ANY)] * n


def solution(mesh):
    n_stage = mesh.shape['stage']
    n_data = mesh.shape['data']
    n_pos = n_stage * n_data

    def per_device(inputs, targets, w_up, w_down):
        n_micro, n_tok, width = inputs.shape
        ffn = w_up.shape[2]
        total = n_data * n_micro * n_tok
        n_chunk = total // CHUNK
        n_tile = ffn // TILE
        inv_total = 1.0 / total
        x = jnp.swapaxes(inputs, 1, 2)
        y = jnp.swapaxes(targets, 1, 2)
        w2 = jnp.swapaxes(w_down, 1, 2)
        dma = pltpu.SemaphoreType.DMA
        flops = 4 * total * width * ffn
        cost = pl.CostEstimate(flops=flops, bytes_accessed=400_000_000, transcendentals=total * ffn)
        act = jax.ShapeDtypeStruct((width, total), BF16)
        hid = jax.ShapeDtypeStruct((total, ffn), BF16)

        h_all, u_all, g_all, e_all, _, loss = pl.pallas_call(
            functools.partial(fwd_kernel, n_pos, n_chunk, inv_total),
            out_shape=(act, jax.ShapeDtypeStruct((total, ffn), F32), hid, act, act,
                       jax.ShapeDtypeStruct((8, CHUNK), F32)),
            in_specs=any_specs(4),
            out_specs=tuple(any_specs(5)) + (pl.BlockSpec(memory_space=pltpu.VMEM),),
            scratch_shapes=[
                pltpu.VMEM((width, ffn), BF16), pltpu.VMEM((width, ffn), BF16),
                pltpu.VMEM((SLOTS, width, CHUNK), BF16), pltpu.VMEM((CHUNK, width), BF16),
                pltpu.VMEM((CHUNK, ffn), F32), pltpu.VMEM((CHUNK, ffn), BF16),
                pltpu.VMEM((width, CHUNK), F32), pltpu.VMEM((2, width, CHUNK), BF16),
                pltpu.VMEM((width, CHUNK), BF16),
                dma((2, n_tile)), dma((SLOTS,)), dma((SLOTS,)), dma((n_tile,)), dma((n_tile,)), dma((2,)), dma,
                dma((SLOTS,)), dma((n_chunk,)), dma((n_chunk,)), dma((n_chunk // 4,)), dma((n_chunk // 4,)),
                pltpu.SemaphoreType.REGULAR,
            ],
            compiler_params=pltpu.CompilerParams(has_side_effects=True, vmem_limit_bytes=VMEM_LIMIT),
            cost_estimate=cost, name='forward_pipe',
        )(x, y, w_up, w2)

        q_all, e_all = pl.pallas_call(
            functools.partial(bwd_kernel, n_pos, n_chunk),
            out_shape=(hid, act),
            in_specs=any_specs(4),
            out_specs=tuple(any_specs(2)),
            input_output_aliases={3: 1},
            scratch_shapes=[
                pltpu.VMEM((width, ffn), BF16), pltpu.VMEM((width, ffn), BF16),
                pltpu.VMEM((SLOTS, width, CHUNK), BF16), pltpu.VMEM((CHUNK, width), BF16),
                pltpu.VMEM((CHUNK, ffn), F32), pltpu.VMEM((CHUNK, ffn), BF16),
                pltpu.VMEM((width, CHUNK), F32), pltpu.VMEM((2, width, CHUNK), BF16),
                dma((2, n_tile)), dma((SLOTS,)), dma((SLOTS,)), dma((n_tile,)), dma((n_tile,)), dma((2,)),
                dma((SLOTS,)), pltpu.SemaphoreType.REGULAR,
            ],
            compiler_params=pltpu.CompilerParams(has_side_effects=True, vmem_limit_bytes=VMEM_LIMIT),
            cost_estimate=cost, name='backward_pipe',
        )(w_up, w2, u_all, e_all)

        stage_id = lax.axis_index('stage')
        data_id = lax.axis_index('data')
        part = width // n_data

        def grad_piece(left, right, first, rows):
            part_of_left = lax.dynamic_slice_in_dim(left, first, rows, 0)
            return jnp.dot(part_of_left, right, preferred_element_type=F32)

        def exchange(piece, k):
            return lax.ppermute(piece, 'data', [(d, d ^ k) for d in range(n_data)]) if k else piece

        def gradient(left, right, cuts):
            out = jnp.zeros((n_data, part, ffn), F32)
            for k in (2, 3, 1, 0):
                slot = (data_id ^ k ^ (2 * stage_id)) % n_data
                at = 0
                for rows in cuts if k == 2 else (part,):
                    piece = grad_piece(left, right, (data_id ^ k) * part + at, rows)
                    out = lax.dynamic_update_slice(out, exchange(piece, k)[None], (slot, at, 0))
                    at += rows
            return out

        grad_up = gradient(h_all, q_all, (128, part - 128))
        grad_down = gradient(e_all, g_all, (part,))
        loss_total = lax.psum(jnp.sum(loss), ('stage', 'data')) * (0.5 * inv_total)
        return loss_total, grad_up, jnp.swapaxes(grad_down, 1, 2)

    return jax.shard_map(
        per_device, mesh=mesh,
        in_specs=(P('data', None, None), P('data', None, None), P('stage', None, None), P('stage', None, None)),
        out_specs=(P(), P('stage', 'data', None), P('stage', None, 'data')), check_vma=False)
```

```python
import functools

import jax
import jax.numpy as jnp
from jax import lax
from jax.experimental import pallas as pl
from jax.experimental.pallas import tpu as pltpu
from jax.sharding import PartitionSpec as P

BF16 = jnp.bfloat16
F32 = jnp.float32
CHUNK = 256
TILE = 1280
SLOTS = 3
MESH = pl.DeviceIdType.MESH
NN = (((1,), (0,)), ((), ()))
NT = (((1,), (1,)), ((), ()))
GELU_A = 0.7978845608028654
GELU_B = 0.044715
VMEM_LIMIT = 66_000_000


def pipe_index(stage, data):
    return 4 * stage + lax.rem(data + 2 * stage, 4)


def pipe_device(pos):
    stage = lax.div(pos, 4)
    return {'stage': stage, 'data': lax.rem(pos + 2 * stage, 4)}


def remote(src, dst, send_sem, recv_sem, pos):
    return pltpu.make_async_remote_copy(
        src_ref=src, dst_ref=dst, send_sem=send_sem, recv_sem=recv_sem,
        device_id=pipe_device(pos), device_id_type=MESH)


def load_weights(layer, pairs, sems, n_tile):
    def copy(i, ref, buf, j):
        part = (slice(None), pl.ds(j * TILE, TILE))
        return pltpu.make_async_copy(ref.at[(layer,) + part], buf.at[part], sems.at[i, j])
    copies = [copy(i, ref, buf, j) for i, (ref, buf) in enumerate(pairs) for j in range(n_tile)]
    for c in copies:
        c.start()
    return copies


def cols(c):
    return pl.ds(pl.multiple_of(c * CHUNK, CHUNK), CHUNK)


def pipe_kernel(n_pos, n_chunk, inv_total,
                x_ref, y_ref, w1_ref, w2_ref,
                h_all, u_all, g_all, q_all, e_all, y_all, loss_ref,
                w1, w2, inbuf, row, ubuf, gbuf, acc, obuf, ybuf, lbuf,
                w_sem, load_sem, store_sem, u_sem, g_sem, out_sem, y_load_sem,
                h_recv_sem, e_recv_sem, x_recv_sem, y_recv_sem, x_send_sem, y_send_sem,
                loss_send_sem, loss_recv_sem, h_credit, e_credit):
    stage = lax.axis_index('stage')
    data = lax.axis_index('data')
    pos = pipe_index(stage, data)
    last = n_pos - 1
    per = n_chunk // 4
    width, ffn = w1.shape
    n_tile = ffn // TILE

    weights = load_weights(lax.rem(pos, 4), ((w1_ref, w1), (w2_ref, w2)), w_sem, n_tile)

    def piece(ref, k):
        n_half = ref.shape[2] // CHUNK
        return ref.at[lax.div(k, n_half), :, cols(lax.rem(k, n_half))]

    def send_x(k):
        c = data * per + k
        return remote(piece(x_ref, k), h_all.at[:, cols(c)], x_send_sem.at[k], x_recv_sem.at[c], 0)

    def send_y(k):
        c = data * per + k
        return remote(piece(y_ref, k), y_all.at[:, cols(c)], y_send_sem.at[k], y_recv_sem.at[c], last)

    def wait_x(c):
        k = lax.rem(c, per)
        remote(piece(x_ref, k), h_all.at[:, cols(c)], x_send_sem.at[k], x_recv_sem.at[c], 0).wait_recv()

    def wait_y(c):
        k = lax.rem(c, per)
        remote(piece(y_ref, k), y_all.at[:, cols(c)], y_send_sem.at[k], y_recv_sem.at[c], last).wait_recv()

    def load(ref, c):
        slot = lax.rem(c, SLOTS)
        return pltpu.make_async_copy(ref.at[:, cols(c)], inbuf.at[slot], load_sem.at[slot])

    def start_x(c):
        slot = lax.rem(c, SLOTS)

        @pl.when(c < per)
        def _():
            pltpu.make_async_copy(piece(x_ref, c), inbuf.at[slot], load_sem.at[slot]).start()

        @pl.when(c >= per)
        def _():
            wait_x(c)
            load(h_all, c).start()

    def y_load(c):
        return pltpu.make_async_copy(y_all.at[:, cols(c)], ybuf, y_load_sem)

    def start_y(c):
        @pl.when(lax.div(c, per) == data)
        def _():
            pltpu.make_async_copy(piece(y_ref, lax.rem(c, per)), ybuf, y_load_sem).start()

        @pl.when(lax.div(c, per) != data)
        def _():
            wait_y(c)
            y_load(c).start()

    def store(ref, c):
        slot = lax.rem(c, SLOTS)
        return pltpu.make_async_copy(inbuf.at[slot], ref.at[:, cols(c)], store_sem.at[slot])

    def send_h(c):
        slot = lax.rem(c, SLOTS)
        out = lax.rem(c, 2)
        return remote(obuf.at[out], inbuf.at[slot], out_sem.at[out], h_recv_sem.at[slot], pos + 1)

    def send_e(c):
        slot = lax.rem(c, SLOTS)
        out = lax.rem(c, 2)
        return remote(obuf.at[out], inbuf.at[slot], out_sem.at[out], e_recv_sem.at[slot], pos - 1)

    def keep_e(c):
        out = lax.rem(c, 2)
        return pltpu.make_async_copy(obuf.at[out], e_all.at[:, cols(c)], out_sem.at[out])

    def u_copy(c, j):
        part = pl.ds(j * TILE, TILE)
        return ubuf.at[:, part], u_all.at[cols(c), part], u_sem.at[j]

    def u_store(c, j):
        vmem, hbm, sem = u_copy(c, j)
        return pltpu.make_async_copy(vmem, hbm, sem)

    def u_load(c, j):
        vmem, hbm, sem = u_copy(c, j)
        return pltpu.make_async_copy(hbm, vmem, sem)

    def g_store(ref, c, j):
        part = pl.ds(j * TILE, TILE)
        return pltpu.make_async_copy(gbuf.at[:, part], ref.at[cols(c), part], g_sem.at[j])

    def send_loss(k):
        return remote(lbuf, loss_ref, loss_send_sem.at[k], loss_recv_sem, k)

    @pl.when((stage == 0) & (pos != 0))
    def _():
        @pl.loop(0, per)
        def _(k):
            send_x(k).start()

    @pl.when((pos == 4) | (pos == 6))
    def _():
        @pl.loop(0, per)
        def _(k):
            send_y(k).start()

    @pl.when(pos == 0)
    def _():
        start_x(0)

    lbuf[...] = jnp.zeros_like(lbuf)
    for copy in weights:
        copy.wait()

    @pl.loop(0, n_chunk)
    def _(c):
        slot = lax.rem(c, SLOTS)

        @pl.when(pos == 0)
        def _():
            load(h_all, c).wait()

            @pl.when(c + 1 < n_chunk)
            def _():
                start_x(c + 1)

        @pl.when(pos != 0)
        def _():
            send_h(c).wait_recv()

        @pl.when((pos != 0) | (c < per))
        def _():
            store(h_all, c).start()

        @pl.when((c > 0) & ((pos != 0) | (c <= per)))
        def _():
            store(h_all, c - 1).wait()

        @pl.when((pos != 0) & (c > 0) & (c - 1 + SLOTS < n_chunk))
        def _():
            pl.semaphore_signal(h_credit, inc=1, device_id=pipe_device(pos - 1), device_id_type=MESH)

        @pl.when(c > 0)
        def _():
            for j in range(n_tile):
                u_store(c - 1, j).wait()
                g_store(g_all, c - 1, j).wait()

        @pl.when(pos == last)
        def _():
            start_y(c)

        row[...] = inbuf[slot].T
        acc[...] = inbuf[slot].astype(F32)
        for j in range(n_tile):
            part = slice(j * TILE, (j + 1) * TILE)
            u = lax.dot_general(row[...], w1[:, part], NN, preferred_element_type=F32)
            ubuf[:, part] = u
            t = jnp.tanh(GELU_A * (u + GELU_B * (u * u * u)))
            gbuf[:, part] = (0.5 * u * (1.0 + t)).astype(BF16)
            u_store(c, j).start()
            g_store(g_all, c, j).start()
            acc[...] += lax.dot_general(w2[:, part], gbuf[:, part], NT, preferred_element_type=F32)

        @pl.when(pos != last)
        def _():
            @pl.when(c > 1)
            def _():
                send_h(c - 2).wait_send()
            obuf[lax.rem(c, 2)] = acc[...].astype(BF16)

            @pl.when(c >= SLOTS)
            def _():
                pl.semaphore_wait(h_credit, 1)
            send_h(c).start()

        @pl.when(pos == last)
        def _():
            @pl.when(c > 1)
            def _():
                keep_e(c - 2).wait()
            y_load(c).wait()
            diff = acc[...].astype(BF16).astype(F32) - ybuf[...].astype(F32)
            lbuf[...] += jnp.sum((diff * diff).reshape(width // 8, 8, CHUNK), axis=0)
            obuf[lax.rem(c, 2)] = (diff * inv_total).astype(BF16)
            keep_e(c).start()

        @pl.when((pos == 5) & (lax.rem(c, 3) == 1) & (c < 3 * per))
        def _():
            send_y(lax.div(c, 3)).start()

    for j in range(n_tile):
        u_store(n_chunk - 1, j).wait()
        g_store(g_all, n_chunk - 1, j).wait()
    for j in range(n_tile):
        u_load(0, j).start()

    @pl.when(pos != 0)
    def _():
        store(h_all, n_chunk - 1).wait()

    @pl.when(pos != last)
    def _():
        for c in (n_chunk - 2, n_chunk - 1):
            send_h(c).wait_send()
        pl.semaphore_signal(e_credit, inc=SLOTS, device_id=pipe_device(pos + 1), device_id_type=MESH)

    @pl.when(pos == last)
    def _():
        for c in (n_chunk - 2, n_chunk - 1):
            keep_e(c).wait()
        load(e_all, 0).start()

        @pl.loop(0, last)
        def _(k):
            send_loss(k).start()

    @pl.loop(0, n_chunk)
    def _(c):
        slot = lax.rem(c, SLOTS)

        @pl.when(pos == last)
        def _():
            load(e_all, c).wait()

            @pl.when(c + 1 < n_chunk)
            def _():
                load(e_all, c + 1).start()

        @pl.when(pos != last)
        def _():
            send_e(c).wait_recv()
            store(e_all, c).start()

            @pl.when(c > 0)
            def _():
                store(e_all, c - 1).wait()

                @pl.when(c - 1 + SLOTS < n_chunk)
                def _():
                    pl.semaphore_signal(e_credit, inc=1, device_id=pipe_device(pos + 1), device_id_type=MESH)

        @pl.when(c > 0)
        def _():
            for j in range(n_tile):
                g_store(q_all, c - 1, j).wait()

        for j in range(n_tile):
            u_load(c, j).wait()

        row[...] = inbuf[slot].T
        acc[...] = inbuf[slot].astype(F32)
        for j in range(n_tile):
            part = slice(j * TILE, (j + 1) * TILE)
            p = lax.dot_general(row[...], w2[:, part], NN, preferred_element_type=F32)
            p = p.astype(BF16).astype(F32)
            u = ubuf[:, part]
            u2 = u * u
            t = jnp.tanh(GELU_A * (u + GELU_B * (u * u2)))
            slope = 0.5 * (1.0 + t) + (0.5 * u) * (1.0 - t * t) * (GELU_A * (1.0 + (3.0 * GELU_B) * u2))
            gbuf[:, part] = (p * slope).astype(BF16)
            g_store(q_all, c, j).start()

            @pl.when(c + 1 < n_chunk)
            def _():
                u_load(c + 1, j).start()
            acc[...] += lax.dot_general(w1[:, part], gbuf[:, part], NT, preferred_element_type=F32)

        @pl.when(pos != 0)
        def _():
            @pl.when(c > 1)
            def _():
                send_e(c - 2).wait_send()
            obuf[lax.rem(c, 2)] = acc[...].astype(BF16)
            pl.semaphore_wait(e_credit, 1)
            send_e(c).start()

    for j in range(n_tile):
        g_store(q_all, n_chunk - 1, j).wait()

    @pl.when(pos != last)
    def _():
        store(e_all, n_chunk - 1).wait()
        send_loss(pos).wait_recv()

    @pl.when(pos == last)
    def _():
        @pl.loop(0, last)
        def _(k):
            send_loss(k).wait_send()
        mine = pltpu.make_async_copy(lbuf, loss_ref, y_load_sem)
        mine.start()
        mine.wait()

    @pl.when(pos != 0)
    def _():
        for c in (n_chunk - 2, n_chunk - 1):
            send_e(c).wait_send()

    @pl.when((stage == 0) & (pos != 0))
    def _():
        @pl.loop(0, per)
        def _(k):
            send_x(k).wait_send()

    @pl.when((stage == 1) & (pos != last))
    def _():
        @pl.loop(0, per)
        def _(k):
            send_y(k).wait_send()


def any_specs(n):
    return [pl.BlockSpec(memory_space=pl.ANY)] * n


def solution(mesh):
    n_stage = mesh.shape['stage']
    n_data = mesh.shape['data']
    n_pos = n_stage * n_data

    def per_device(inputs, targets, w_up, w_down):
        n_micro, n_tok, width = inputs.shape
        ffn = w_up.shape[2]
        total = n_data * n_micro * n_tok
        n_chunk = total // CHUNK
        n_tile = ffn // TILE
        inv_total = 1.0 / total
        x = jnp.swapaxes(inputs, 1, 2)
        y = jnp.swapaxes(targets, 1, 2)
        w2 = jnp.swapaxes(w_down, 1, 2)
        dma = pltpu.SemaphoreType.DMA
        flops = 8 * total * width * ffn
        cost = pl.CostEstimate(flops=flops, bytes_accessed=1_000_000_000, transcendentals=2 * total * ffn)
        act = jax.ShapeDtypeStruct((width, total), BF16)
        hid = jax.ShapeDtypeStruct((total, ffn), BF16)

        h_all, _, g_all, q_all, e_all, _, loss = pl.pallas_call(
            functools.partial(pipe_kernel, n_pos, n_chunk, inv_total),
            out_shape=(act, jax.ShapeDtypeStruct((total, ffn), F32), hid, hid, act, act,
                       jax.ShapeDtypeStruct((8, CHUNK), F32)),
            in_specs=any_specs(4),
            out_specs=tuple(any_specs(7)),
            scratch_shapes=[
                pltpu.VMEM((width, ffn), BF16), pltpu.VMEM((width, ffn), BF16),
                pltpu.VMEM((SLOTS, width, CHUNK), BF16), pltpu.VMEM((CHUNK, width), BF16),
                pltpu.VMEM((CHUNK, ffn), F32), pltpu.VMEM((CHUNK, ffn), BF16),
                pltpu.VMEM((width, CHUNK), F32), pltpu.VMEM((2, width, CHUNK), BF16),
                pltpu.VMEM((width, CHUNK), BF16), pltpu.VMEM((8, CHUNK), F32),
                dma((2, n_tile)), dma((SLOTS,)), dma((SLOTS,)), dma((n_tile,)), dma((n_tile,)), dma((2,)), dma,
                dma((SLOTS,)), dma((SLOTS,)), dma((n_chunk,)), dma((n_chunk,)),
                dma((n_chunk // 4,)), dma((n_chunk // 4,)), dma((n_pos,)), dma,
                pltpu.SemaphoreType.REGULAR, pltpu.SemaphoreType.REGULAR,
            ],
            compiler_params=pltpu.CompilerParams(has_side_effects=True, vmem_limit_bytes=VMEM_LIMIT),
            cost_estimate=cost, name='pipe',
        )(x, y, w_up, w2)

        stage_id = lax.axis_index('stage')
        data_id = lax.axis_index('data')
        part = width // n_data

        def grad_piece(left, right, first, rows):
            part_of_left = lax.dynamic_slice_in_dim(left, first, rows, 0)
            return jnp.dot(part_of_left, right, preferred_element_type=F32)

        def exchange(piece, k):
            return lax.ppermute(piece, 'data', [(d, d ^ k) for d in range(n_data)]) if k else piece

        def gradient(left, right, cuts, order):
            made = []
            for k in (2, 3, 1, 0):
                at = 0
                for rows in cuts if k == 2 else (part,):
                    piece = grad_piece(left, right, (data_id ^ k) * part + at, rows)
                    made.append((k, at, exchange(piece, k)))
                    at += rows
            out = jnp.zeros((n_data, part, ffn), F32)
            for k, at, piece in sorted(made, key=lambda m: order.index(m[0])):
                slot = (data_id ^ k ^ (2 * stage_id)) % n_data
                out = lax.dynamic_update_slice(out, piece[None], (slot, at, 0))
            return out

        grad_up = gradient(h_all, q_all, (128, part - 128), (0, 2, 3, 1))
        grad_down = gradient(e_all, g_all, (part,), (0, 2, 3, 1))
        loss_total = jnp.sum(loss) * (0.5 * inv_total)
        return loss_total, grad_up, jnp.swapaxes(grad_down, 1, 2)

    return jax.shard_map(
        per_device, mesh=mesh,
        in_specs=(P('data', None, None), P('data', None, None), P('stage', None, None), P('stage', None, None)),
        out_specs=(P(), P('stage', 'data', None), P('stage', None, 'data')), check_vma=False)
```

```python
import functools

import jax
import jax.numpy as jnp
from jax import lax
from jax.experimental import pallas as pl
from jax.experimental.pallas import tpu as pltpu
from jax.sharding import PartitionSpec as P

BF16 = jnp.bfloat16
F32 = jnp.float32
CHUNK = 256
TILE = 1280
SLOTS = 3
DEEP = 2048
OUTER_TILES = 2
MESH = pl.DeviceIdType.MESH
NN = (((1,), (0,)), ((), ()))
NT = (((1,), (1,)), ((), ()))
GELU_A = 0.7978845608028654
GELU_B = 0.044715
VMEM_LIMIT = 66_000_000


def pipe_index(stage, data):
    return 4 * stage + lax.rem(data + 2 * stage, 4)


def pipe_device(pos):
    stage = lax.div(pos, 4)
    return {'stage': stage, 'data': lax.rem(pos + 2 * stage, 4)}


def remote(src, dst, send_sem, recv_sem, pos):
    return pltpu.make_async_remote_copy(
        src_ref=src, dst_ref=dst, send_sem=send_sem, recv_sem=recv_sem,
        device_id=pipe_device(pos), device_id_type=MESH)


def load_weights(layer, pairs, sems, n_tile):
    def copy(i, ref, buf, j):
        part = (slice(None), pl.ds(j * TILE, TILE))
        return pltpu.make_async_copy(ref.at[(layer,) + part], buf.at[part], sems.at[i, j])
    copies = [copy(i, ref, buf, j) for i, (ref, buf) in enumerate(pairs) for j in range(n_tile)]
    for c in copies:
        c.start()
    return copies


def cols(c):
    return pl.ds(pl.multiple_of(c * CHUNK, CHUNK), CHUNK)


def pipe_kernel(n_pos, n_chunk, inv_total,
                x_ref, y_ref, w1_ref, w2_ref,
                h_all, u_all, g_all, q_all, e_all, y_all, loss_ref, hd_all, ed_lo, ed_hi, e_hi,
                w1, w2, inbuf, row, ubuf, gbuf, acc, obuf, ybuf, lbuf,
                w_sem, load_sem, store_sem, u_sem, g_sem, out_sem, y_load_sem,
                h_recv_sem, e_recv_sem, x_recv_sem, y_recv_sem, x_send_sem, y_send_sem,
                loss_send_sem, loss_recv_sem, keep_sem, far_sem, hd_send_sem, hd_recv_sem, ed_send_sem, ed_recv_sem,
                h_credit, e_credit):
    stage = lax.axis_index('stage')
    data = lax.axis_index('data')
    pos = pipe_index(stage, data)
    last = n_pos - 1
    per = n_chunk // 4
    width, ffn = w1.shape
    n_tile = ffn // TILE

    weights = load_weights(lax.rem(pos, 4), ((w1_ref, w1), (w2_ref, w2)), w_sem, n_tile)

    def piece(ref, k):
        n_half = ref.shape[2] // CHUNK
        return ref.at[lax.div(k, n_half), :, cols(lax.rem(k, n_half))]

    def send_x(k):
        c = data * per + k
        return remote(piece(x_ref, k), h_all.at[:, cols(c)], x_send_sem.at[k], x_recv_sem.at[c], 0)

    def send_y(k):
        c = data * per + k
        return remote(piece(y_ref, k), y_all.at[:, cols(c)], y_send_sem.at[k], y_recv_sem.at[c], last)

    def wait_x(c):
        k = lax.rem(c, per)
        remote(piece(x_ref, k), h_all.at[:, cols(c)], x_send_sem.at[k], x_recv_sem.at[c], 0).wait_recv()

    def wait_y(c):
        k = lax.rem(c, per)
        remote(piece(y_ref, k), y_all.at[:, cols(c)], y_send_sem.at[k], y_recv_sem.at[c], last).wait_recv()

    def load(ref, c):
        slot = lax.rem(c, SLOTS)
        return pltpu.make_async_copy(ref.at[:, cols(c)], inbuf.at[slot], load_sem.at[slot])

    def start_x(c):
        slot = lax.rem(c, SLOTS)

        @pl.when(c < per)
        def _():
            pltpu.make_async_copy(piece(x_ref, c), inbuf.at[slot], load_sem.at[slot]).start()

        @pl.when(c >= per)
        def _():
            wait_x(c)
            load(h_all, c).start()

    def y_load(c):
        return pltpu.make_async_copy(y_all.at[:, cols(c)], ybuf, y_load_sem)

    def start_y(c):
        @pl.when(lax.div(c, per) == data)
        def _():
            pltpu.make_async_copy(piece(y_ref, lax.rem(c, per)), ybuf, y_load_sem).start()

        @pl.when(lax.div(c, per) != data)
        def _():
            wait_y(c)
            y_load(c).start()

    def store(ref, c):
        slot = lax.rem(c, SLOTS)
        return pltpu.make_async_copy(inbuf.at[slot], ref.at[:, cols(c)], store_sem.at[slot])

    def send_h(c):
        slot = lax.rem(c, SLOTS)
        out = lax.rem(c, 2)
        return remote(obuf.at[out], inbuf.at[slot], out_sem.at[out], h_recv_sem.at[slot], pos + 1)

    def send_e(c):
        slot = lax.rem(c, SLOTS)
        out = lax.rem(c, 2)
        return remote(obuf.at[out], inbuf.at[slot], out_sem.at[out], e_recv_sem.at[slot], pos - 1)

    def keep_e(c):
        out = lax.rem(c, 2)
        return pltpu.make_async_copy(obuf.at[out], e_all.at[:, cols(c)], out_sem.at[out])

    def u_copy(c, j):
        part = pl.ds(j * TILE, TILE)
        return ubuf.at[:, part], u_all.at[cols(c), part], u_sem.at[j]

    def u_store(c, j):
        vmem, hbm, sem = u_copy(c, j)
        return pltpu.make_async_copy(vmem, hbm, sem)

    def u_load(c, j):
        vmem, hbm, sem = u_copy(c, j)
        return pltpu.make_async_copy(hbm, vmem, sem)

    def g_store(ref, c, j):
        part = pl.ds(j * TILE, TILE)
        return pltpu.make_async_copy(gbuf.at[:, part], ref.at[cols(c), part], g_sem.at[j])

    role = lax.rem(pos, 4)
    inner_up = role == 1
    inner_down = role == 2
    half = n_chunk // 2
    narrow = CHUNK // 2

    def thin(k):
        return pl.ds(pl.multiple_of(k * narrow, narrow), narrow)

    def keep_h(c):
        out = lax.rem(c, 2)
        return pltpu.make_async_copy(obuf.at[out], hd_all.at[:, cols(c)], keep_sem.at[out])

    def keep_far(ref, c):
        out = lax.rem(c, 2)
        return pltpu.make_async_copy(obuf.at[out], ref.at[:, cols(lax.rem(c, half))], keep_sem.at[out])

    def store_hi(c):
        slot = lax.rem(c, SLOTS)
        return pltpu.make_async_copy(inbuf.at[slot], e_hi.at[:, cols(lax.rem(c, half))], far_sem.at[slot])

    def send_hd(k):
        return remote(h_all.at[:, cols(k)], hd_all.at[:, cols(k)], hd_send_sem.at[k], hd_recv_sem.at[k], pos + 1)

    def send_ed(k):
        return remote(e_all.at[:, thin(k)], ed_lo.at[:, thin(k)], ed_send_sem.at[k], ed_recv_sem.at[k], pos - 1)

    def send_loss(k):
        return remote(lbuf, loss_ref, loss_send_sem.at[k], loss_recv_sem, k)

    @pl.when((stage == 0) & (pos != 0))
    def _():
        @pl.loop(0, per)
        def _(k):
            send_x(k).start()

    @pl.when((pos == 4) | (pos == 6))
    def _():
        @pl.loop(0, per)
        def _(k):
            send_y(k).start()

    @pl.when(pos == 0)
    def _():
        start_x(0)

    lbuf[...] = jnp.zeros_like(lbuf)
    for copy in weights:
        copy.wait()

    @pl.loop(0, n_chunk)
    def _(c):
        slot = lax.rem(c, SLOTS)

        @pl.when(pos == 0)
        def _():
            load(h_all, c).wait()

            @pl.when(c + 1 < n_chunk)
            def _():
                start_x(c + 1)

        @pl.when(pos != 0)
        def _():
            send_h(c).wait_recv()

        @pl.when((pos != 0) | (c < per))
        def _():
            store(h_all, c).start()

        @pl.when((c > 0) & ((pos != 0) | (c <= per)))
        def _():
            store(h_all, c - 1).wait()

        @pl.when((pos != 0) & (c > 0) & (c - 1 + SLOTS < n_chunk))
        def _():
            pl.semaphore_signal(h_credit, inc=1, device_id=pipe_device(pos - 1), device_id_type=MESH)

        @pl.when(c > 0)
        def _():
            for j in range(n_tile):
                u_store(c - 1, j).wait()
                g_store(g_all, c - 1, j).wait()

        @pl.when(pos == last)
        def _():
            start_y(c)

        row[...] = inbuf[slot].T
        acc[...] = inbuf[slot].astype(F32)
        for j in range(n_tile):
            part = slice(j * TILE, (j + 1) * TILE)
            u = lax.dot_general(row[...], w1[:, part], NN, preferred_element_type=F32)
            ubuf[:, part] = u
            t = jnp.tanh(GELU_A * (u + GELU_B * (u * u * u)))
            gbuf[:, part] = (0.5 * u * (1.0 + t)).astype(BF16)
            u_store(c, j).start()
            g_store(g_all, c, j).start()
            acc[...] += lax.dot_general(w2[:, part], gbuf[:, part], NT, preferred_element_type=F32)

        @pl.when(pos != last)
        def _():
            @pl.when(c > 1)
            def _():
                send_h(c - 2).wait_send()

            @pl.when((c > 1) & inner_up)
            def _():
                keep_h(c - 2).wait()
            obuf[lax.rem(c, 2)] = acc[...].astype(BF16)

            @pl.when(c >= SLOTS)
            def _():
                pl.semaphore_wait(h_credit, 1)
            send_h(c).start()

            @pl.when(inner_up)
            def _():
                keep_h(c).start()

        @pl.when(pos == last)
        def _():
            @pl.when(c > 1)
            def _():
                keep_e(c - 2).wait()
            y_load(c).wait()
            diff = acc[...].astype(BF16).astype(F32) - ybuf[...].astype(F32)
            lbuf[...] += jnp.sum((diff * diff).reshape(width // 8, 8, CHUNK), axis=0)
            obuf[lax.rem(c, 2)] = (diff * inv_total).astype(BF16)
            keep_e(c).start()

        @pl.when((pos == 5) & (lax.rem(c, 3) == 1) & (c < 3 * per))
        def _():
            send_y(lax.div(c, 3)).start()

    for j in range(n_tile):
        u_store(n_chunk - 1, j).wait()
        g_store(g_all, n_chunk - 1, j).wait()
    for j in range(n_tile):
        u_load(0, j).start()

    @pl.when(pos != 0)
    def _():
        store(h_all, n_chunk - 1).wait()

    @pl.when(pos != last)
    def _():
        for c in (n_chunk - 2, n_chunk - 1):
            send_h(c).wait_send()
        pl.semaphore_signal(e_credit, inc=SLOTS, device_id=pipe_device(pos + 1), device_id_type=MESH)

    @pl.when(inner_up)
    def _():
        for c in (n_chunk - 2, n_chunk - 1):
            keep_h(c).wait()

        @pl.loop(0, n_chunk)
        def _(k):
            send_hd(k).start()

    @pl.when(pos == last)
    def _():
        for c in (n_chunk - 2, n_chunk - 1):
            keep_e(c).wait()
        load(e_all, 0).start()

        @pl.loop(0, last)
        def _(k):
            send_loss(k).start()

    @pl.loop(0, n_chunk)
    def _(c):
        slot = lax.rem(c, SLOTS)

        @pl.when(pos == last)
        def _():
            load(e_all, c).wait()

            @pl.when(c + 1 < n_chunk)
            def _():
                load(e_all, c + 1).start()

        @pl.when(pos != last)
        def _():
            send_e(c).wait_recv()
            store(e_all, c).start()

            @pl.when(inner_down & (c >= half))
            def _():
                store_hi(c).start()

            @pl.when(inner_down & (c > half))
            def _():
                store_hi(c - 1).wait()

            @pl.when(c > 0)
            def _():
                store(e_all, c - 1).wait()

                @pl.when(c - 1 + SLOTS < n_chunk)
                def _():
                    pl.semaphore_signal(e_credit, inc=1, device_id=pipe_device(pos + 1), device_id_type=MESH)

        @pl.when(c > 0)
        def _():
            for j in range(n_tile):
                g_store(q_all, c - 1, j).wait()

        for j in range(n_tile):
            u_load(c, j).wait()

        row[...] = inbuf[slot].T
        acc[...] = inbuf[slot].astype(F32)
        for j in range(n_tile):
            part = slice(j * TILE, (j + 1) * TILE)
            p = lax.dot_general(row[...], w2[:, part], NN, preferred_element_type=F32)
            p = p.astype(BF16).astype(F32)
            u = ubuf[:, part]
            u2 = u * u
            t = jnp.tanh(GELU_A * (u + GELU_B * (u * u2)))
            slope = 0.5 * (1.0 + t) + (0.5 * u) * (1.0 - t * t) * (GELU_A * (1.0 + (3.0 * GELU_B) * u2))
            gbuf[:, part] = (p * slope).astype(BF16)
            g_store(q_all, c, j).start()

            @pl.when(c + 1 < n_chunk)
            def _():
                u_load(c + 1, j).start()
            acc[...] += lax.dot_general(w1[:, part], gbuf[:, part], NT, preferred_element_type=F32)

        @pl.when(pos != 0)
        def _():
            @pl.when(c > 1)
            def _():
                send_e(c - 2).wait_send()

            @pl.when((c > 1) & inner_down)
            def _():
                keep_far(ed_lo, c - 2).wait()
            obuf[lax.rem(c, 2)] = acc[...].astype(BF16)
            pl.semaphore_wait(e_credit, 1)
            send_e(c).start()

            @pl.when(inner_down & (c < half))
            def _():
                keep_far(ed_lo, c).start()

            @pl.when(inner_down & (c >= half))
            def _():
                keep_far(ed_hi, c).start()

            @pl.when(inner_down & (c > 0))
            def _():
                send_ed(c - 1).start()

    for j in range(n_tile):
        g_store(q_all, n_chunk - 1, j).wait()

    @pl.when(pos != last)
    def _():
        store(e_all, n_chunk - 1).wait()
        send_loss(pos).wait_recv()

    @pl.when(pos == last)
    def _():
        @pl.loop(0, last)
        def _(k):
            send_loss(k).wait_send()
        mine = pltpu.make_async_copy(lbuf, loss_ref, y_load_sem)
        mine.start()
        mine.wait()

    @pl.when(pos != 0)
    def _():
        for c in (n_chunk - 2, n_chunk - 1):
            send_e(c).wait_send()

    @pl.when(inner_down)
    def _():
        store_hi(n_chunk - 1).wait()
        send_ed(n_chunk - 1).start()
        for c in (n_chunk - 2, n_chunk - 1):
            keep_far(ed_hi, c).wait()

        @pl.loop(0, n_chunk)
        def _(k):
            remote(h_all.at[:, cols(k)], hd_all.at[:, cols(k)], hd_send_sem.at[k], hd_recv_sem.at[k], pos - 1).wait_recv()
            send_ed(k).wait_send()

    @pl.when(inner_up)
    def _():
        @pl.loop(0, n_chunk)
        def _(k):
            send_hd(k).wait_send()
            remote(e_all.at[:, thin(k)], ed_lo.at[:, thin(k)], ed_send_sem.at[k], ed_recv_sem.at[k], pos + 1).wait_recv()

    @pl.when((stage == 0) & (pos != 0))
    def _():
        @pl.loop(0, per)
        def _(k):
            send_x(k).wait_send()

    @pl.when((stage == 1) & (pos != last))
    def _():
        @pl.loop(0, per)
        def _(k):
            send_y(k).wait_send()


def redo_kernel(n_chunk, outer_tiles, w1_ref, w2_ref, hd_own, hd_got, lo_own, lo_got, hi_own, hi_tail, hi_got_a, hi_got_b,
                h_all, e_all, g_all, q_all,
                w1, w2, hbuf, ebuf, hrow, erow, gbuf, qbuf, w_sem, h_sem, e_sem, hs_sem, es_sem, g_sem, q_sem):
    stage = lax.axis_index('stage')
    data = lax.axis_index('data')
    role = lax.rem(pipe_index(stage, data), 4)
    inner = (role == 1) | (role == 2)
    up = role < 2
    layer = jnp.where(up, 2, 1)
    n_tile = w1.shape[1] // TILE
    half = n_chunk // 2
    first = jnp.where(inner, outer_tiles * TILE, 0)

    def weight(i, ref, buf, j):
        at = pl.ds(pl.multiple_of(first + j * TILE, TILE), TILE)
        return pltpu.make_async_copy(ref.at[layer, :, at], buf.at[:, pl.ds(j * TILE, TILE)], w_sem.at[i, j])

    def weights(do):
        for j in range(n_tile):
            if j < outer_tiles:
                do(weight(0, w1_ref, w1, j))
                do(weight(1, w2_ref, w2, j))
            else:
                @pl.when(inner)
                def _():
                    do(weight(0, w1_ref, w1, j))
                    do(weight(1, w2_ref, w2, j))

    def h_load(ref, c):
        return pltpu.make_async_copy(ref.at[:, cols(c)], hbuf.at[lax.rem(c, 2)], h_sem.at[lax.rem(c, 2)])

    def e_load(ref, c):
        return pltpu.make_async_copy(ref.at[:, cols(lax.rem(c, half))], ebuf.at[lax.rem(c, 2)], e_sem.at[lax.rem(c, 2)])

    def start_load(c):
        for yes, ref in ((inner, hd_own), (~inner, hd_got)):
            @pl.when(yes)
            def _():
                h_load(ref, c).start()
        low = c < half
        for yes, ref in ((inner & low, lo_own), (~inner & low, lo_got), (~up & inner & ~low, hi_own), (up & inner & ~low, hi_tail),
                         (up & ~inner & ~low, hi_got_a), (~up & ~inner & ~low, hi_got_b)):
            @pl.when(yes)
            def _():
                e_load(ref, c).start()

    def h_store(c):
        return pltpu.make_async_copy(hbuf.at[lax.rem(c, 2)], h_all.at[:, cols(c)], hs_sem.at[lax.rem(c, 2)])

    def e_store(c):
        return pltpu.make_async_copy(ebuf.at[lax.rem(c, 2)], e_all.at[:, cols(c)], es_sem.at[lax.rem(c, 2)])

    def tile_store(buf, ref, sem, c, j):
        part = pl.ds(j * TILE, TILE)
        return pltpu.make_async_copy(buf.at[:, part], ref.at[cols(c), part], sem.at[j])

    def stores(c, do):
        for j in range(n_tile):
            if j < outer_tiles:
                do(tile_store(gbuf, g_all, g_sem, c, j))
                do(tile_store(qbuf, q_all, q_sem, c, j))
            else:
                @pl.when(inner)
                def _():
                    do(tile_store(gbuf, g_all, g_sem, c, j))
                    do(tile_store(qbuf, q_all, q_sem, c, j))

    def wait(copy):
        copy.wait()

    start_load(0)
    weights(lambda copy: copy.start())
    weights(wait)

    @pl.loop(0, n_chunk)
    def _(c):
        slot = lax.rem(c, 2)
        h_load(hd_own, c).wait()
        e_load(lo_own, c).wait()
        h_store(c).start()
        e_store(c).start()

        @pl.when(c > 0)
        def _():
            h_store(c - 1).wait()
            e_store(c - 1).wait()
            stores(c - 1, wait)

        @pl.when(c + 1 < n_chunk)
        def _():
            start_load(c + 1)

        hrow[...] = hbuf[slot].T
        erow[...] = ebuf[slot].T

        def tile(j):
            part = slice(j * TILE, (j + 1) * TILE)
            u = lax.dot_general(hrow[...], w1[:, part], NN, preferred_element_type=F32)
            p = lax.dot_general(erow[...], w2[:, part], NN, preferred_element_type=F32)
            p = p.astype(BF16).astype(F32)
            u2 = u * u
            t = jnp.tanh(GELU_A * (u + GELU_B * (u * u2)))
            gbuf[:, part] = (0.5 * u * (1.0 + t)).astype(BF16)
            slope = 0.5 * (1.0 + t) + (0.5 * u) * (1.0 - t * t) * (GELU_A * (1.0 + (3.0 * GELU_B) * u2))
            qbuf[:, part] = (p * slope).astype(BF16)

        for j in range(outer_tiles):
            tile(j)

        @pl.when(inner)
        def _():
            for j in range(outer_tiles, n_tile):
                tile(j)
        stores(c, lambda copy: copy.start())

    h_store(n_chunk - 1).wait()
    e_store(n_chunk - 1).wait()
    stores(n_chunk - 1, wait)


def grad_kernel(n_alias, at_ref, left_a, left_b, right, *refs):
    out_a, out_b = refs[n_alias:]
    i = pl.program_id(0)
    k = pl.program_id(1)

    @pl.when((i < at_ref[2]) & (k == 0))
    def _():
        out_a[...] = jnp.dot(left_a[...], right[...], preferred_element_type=F32).reshape(out_a.shape)
        out_b[...] = jnp.dot(left_b[...], right[...], preferred_element_type=F32)

    @pl.when((i < at_ref[2]) & (k > 0))
    def _():
        out_a[...] += jnp.dot(left_a[...], right[...], preferred_element_type=F32).reshape(out_a.shape)
        out_b[...] += jnp.dot(left_b[...], right[...], preferred_element_type=F32)


def any_specs(n):
    return [pl.BlockSpec(memory_space=pl.ANY)] * n


def solution(mesh):
    n_stage = mesh.shape['stage']
    n_data = mesh.shape['data']
    n_pos = n_stage * n_data

    def per_device(inputs, targets, w_up, w_down):
        n_micro, n_tok, width = inputs.shape
        ffn = w_up.shape[2]
        total = n_data * n_micro * n_tok
        n_chunk = total // CHUNK
        n_tile = ffn // TILE
        inv_total = 1.0 / total
        x = jnp.swapaxes(inputs, 1, 2)
        y = jnp.swapaxes(targets, 1, 2)
        w2 = jnp.swapaxes(w_down, 1, 2)
        dma = pltpu.SemaphoreType.DMA
        flops = 8 * total * width * ffn
        cost = pl.CostEstimate(flops=flops, bytes_accessed=1_000_000_000, transcendentals=2 * total * ffn)
        act = jax.ShapeDtypeStruct((width, total), BF16)
        half_act = jax.ShapeDtypeStruct((width, total // 2), BF16)
        hid = jax.ShapeDtypeStruct((total, ffn), BF16)

        h_all, _, g_all, q_all, e_all, _, loss, hd_all, ed_lo, ed_hi, e_hi = pl.pallas_call(
            functools.partial(pipe_kernel, n_pos, n_chunk, inv_total),
            out_shape=(act, jax.ShapeDtypeStruct((total, ffn), F32), hid, hid, act, act,
                       jax.ShapeDtypeStruct((8, CHUNK), F32), act, half_act, half_act, half_act),
            in_specs=any_specs(4),
            out_specs=tuple(any_specs(11)),
            scratch_shapes=[
                pltpu.VMEM((width, ffn), BF16), pltpu.VMEM((width, ffn), BF16),
                pltpu.VMEM((SLOTS, width, CHUNK), BF16), pltpu.VMEM((CHUNK, width), BF16),
                pltpu.VMEM((CHUNK, ffn), F32), pltpu.VMEM((CHUNK, ffn), BF16),
                pltpu.VMEM((width, CHUNK), F32), pltpu.VMEM((2, width, CHUNK), BF16),
                pltpu.VMEM((width, CHUNK), BF16), pltpu.VMEM((8, CHUNK), F32),
                dma((2, n_tile)), dma((SLOTS,)), dma((SLOTS,)), dma((n_tile,)), dma((n_tile,)), dma((2,)), dma,
                dma((SLOTS,)), dma((SLOTS,)), dma((n_chunk,)), dma((n_chunk,)),
                dma((n_chunk // 4,)), dma((n_chunk // 4,)), dma((n_pos,)), dma,
                dma((2,)), dma((SLOTS,)), dma((n_chunk,)), dma((n_chunk,)), dma((n_chunk,)), dma((n_chunk,)),
                pltpu.SemaphoreType.REGULAR, pltpu.SemaphoreType.REGULAR,
            ],
            compiler_params=pltpu.CompilerParams(has_side_effects=True, vmem_limit_bytes=VMEM_LIMIT),
            cost_estimate=cost, name='pipe',
        )(x, y, w_up, w2)

        stage_id = lax.axis_index('stage')
        data_id = lax.axis_index('data')
        part = width // n_data
        role = pipe_index(stage_id, data_id) % 4
        inner = (role == 1) | (role == 2)

        def flat(pos):
            return n_data * (pos // n_data) + (pos + 2 * (pos // n_data)) % n_data

        def move(value, pairs):
            return lax.ppermute(value, ('stage', 'data'), [(flat(a + 4 * s), flat(b + 4 * s)) for s in range(n_stage) for a, b in pairs])

        tail = move(e_hi, [(2, 1)])
        hd_got = move(hd_all, [(1, 0), (2, 3)])
        lo_got = move(ed_lo, [(1, 0), (2, 3)])
        hi_got_a = move(tail, [(1, 0)])
        hi_got_b = move(ed_hi, [(2, 3)])

        def gradient(left, right, rows_a, rows_b, n_block, active, slot, col, home=None, final=True):
            at = jnp.stack([rows_a, rows_b, active, slot, col]).astype(jnp.int32)

            def tile(i, at):
                return jnp.maximum(jnp.minimum(i, at[2] - 1), 0)

            def depth(i, k, at):
                return jnp.where(i < at[2], k, jnp.where(at[2] > 0, total // DEEP - 1, 0))

            plain = pl.BlockSpec((part, TILE), lambda i, k, at: (0, tile(i, at)))
            flops = 4 * part * TILE * n_block * total
            kept = [] if home is None else [home]
            out_a = (jax.ShapeDtypeStruct((n_data, part, ffn), F32) if final else jax.ShapeDtypeStruct((part, TILE * n_block), F32))
            return pl.pallas_call(
                functools.partial(grad_kernel, len(kept)),
                out_shape=(out_a, jax.ShapeDtypeStruct((part, TILE * n_block), F32)),
                grid_spec=pltpu.PrefetchScalarGridSpec(
                    num_scalar_prefetch=1, grid=(n_block, total // DEEP),
                    in_specs=[
                        pl.BlockSpec((part, DEEP), lambda i, k, at: (at[0], depth(i, k, at))),
                        pl.BlockSpec((part, DEEP), lambda i, k, at: (at[1], depth(i, k, at))),
                        pl.BlockSpec((DEEP, TILE), lambda i, k, at: (depth(i, k, at), tile(i, at))),
                    ] + any_specs(len(kept)),
                    out_specs=(pl.BlockSpec((1, part, TILE), lambda i, k, at: (at[3], 0, at[4] + tile(i, at))) if final else plain, plain)),
                input_output_aliases={4: 0} if kept else {},
                compiler_params=pltpu.CompilerParams(vmem_limit_bytes=VMEM_LIMIT),
                cost_estimate=pl.CostEstimate(flops=flops, bytes_accessed=flops // 400, transcendentals=0),
                name='gradient',
            )(at, left, left, right, *kept)

        pairs = (('up', h_all, q_all), ('down', e_all, g_all))
        mine, other = data_id, data_id ^ 1
        far = {}
        for name, left, right in pairs:
            a, b = gradient(left, right, data_id ^ 2, data_id ^ 3, n_tile, jnp.where(inner, 0, n_tile), 0, 0, final=False)
            far[name] = (move(a, [(0, 2), (3, 1)]), move(b, [(0, 3), (3, 0)]))
        home = {}
        near = {}
        for name, left, right in pairs:
            home[name], sent = gradient(left, right, mine, other, n_tile, n_tile, role, 0)
            near[name] = move(sent, [(0, 1), (1, 0), (2, 3), (3, 2)])

        n_redo = n_tile - OUTER_TILES
        redo_hid = jax.ShapeDtypeStruct((total, n_redo * TILE), BF16)
        hd, ed, gd, qd = pl.pallas_call(
            functools.partial(redo_kernel, n_chunk, OUTER_TILES),
            out_shape=(act, act, redo_hid, redo_hid),
            in_specs=any_specs(10),
            out_specs=tuple(any_specs(4)),
            scratch_shapes=[
                pltpu.VMEM((width, n_redo * TILE), BF16), pltpu.VMEM((width, n_redo * TILE), BF16),
                pltpu.VMEM((2, width, CHUNK), BF16), pltpu.VMEM((2, width, CHUNK), BF16),
                pltpu.VMEM((CHUNK, width), BF16), pltpu.VMEM((CHUNK, width), BF16),
                pltpu.VMEM((CHUNK, n_redo * TILE), BF16), pltpu.VMEM((CHUNK, n_redo * TILE), BF16),
                dma((2, n_redo)), dma((2,)), dma((2,)), dma((2,)), dma((2,)), dma((n_redo,)), dma((n_redo,)),
            ],
            compiler_params=pltpu.CompilerParams(vmem_limit_bytes=VMEM_LIMIT),
            cost_estimate=pl.CostEstimate(flops=flops // 4, bytes_accessed=400_000_000, transcendentals=total * ffn // 2),
            name='redo',
        )(w_up, w2, hd_all, hd_got, ed_lo, lo_got, ed_hi, tail, hi_got_a, hi_got_b)

        redo_slot = jnp.where(role < 2, 2, 1)
        active = jnp.where(inner, n_redo, OUTER_TILES)
        first = jnp.where(inner, OUTER_TILES, 0)
        redone = {}
        for name, left, right in (('up', hd, qd), ('down', ed, gd)):
            home[name], sent = gradient(left, right, mine, other, n_redo, active, redo_slot, first, home=home[name])
            redone[name] = move(sent, [(0, 1), (1, 0), (2, 3), (3, 2)])

        grads = {}
        for name in home:
            out = home[name]
            out = lax.dynamic_update_slice(out, near[name][None], (role ^ 1, 0, 0))
            got = jnp.where(inner, far[name][0], far[name][1])
            out = lax.dynamic_update_slice(out, got[None], (jnp.where(role < 2, 3, 0), 0, 0))
            at = jnp.where(inner, 0, OUTER_TILES * TILE)
            cut = OUTER_TILES * TILE
            out = lax.dynamic_update_slice(out, redone[name][None, :, :cut], (redo_slot, 0, at))
            mine_end = lax.dynamic_slice(out, (redo_slot, 0, 2 * cut), (1, part, ffn - 2 * cut))
            end = jnp.where(inner, mine_end, redone[name][None, :, cut:])
            grads[name] = lax.dynamic_update_slice(out, end, (redo_slot, 0, 2 * cut))
        grad_up, grad_down = grads['up'], grads['down']
        loss_total = jnp.sum(loss) * (0.5 * inv_total)
        return loss_total, grad_up, jnp.swapaxes(grad_down, 1, 2)

    return jax.shard_map(
        per_device, mesh=mesh,
        in_specs=(P('data', None, None), P('data', None, None), P('stage', None, None), P('stage', None, None)),
        out_specs=(P(), P('stage', 'data', None), P('stage', None, 'data')), check_vma=False)
```
